32 devices in a mesh: gx: 2 (over x), gy: 4 (over z), gz: 4 (over y, core).
Axes of the slice: x: 2, y: 2, z: 4, core: 2. Of those that a mesh axis runs over, the one named last changes fastest.
Arguments:
- velocity: float32 [3, 16, 32, 512], P(None, 'gx', 'gy', 'gz'), may hold values from -6 to 6
- direction: float32 [3, 16, 32, 512], P(None, 'gx', 'gy', 'gz'), may hold values from -3 to 3
- pressure: float32 [16, 32, 512], P('gx', 'gy', 'gz'), may hold values from -6 to 6
- body_force: float32 [3, 16, 32, 512], P(None, 'gx', 'gy', 'gz'), may hold values from -21 to 21, as said below
- phase_ids: int32 [16, 32, 512], P('gx', 'gy', 'gz'), may hold values from 0 to 3
- creep_factor: float32 [4], replicated, may hold values from 0.5 to 2
- stress_exponent: float32 [4], replicated, may hold values from 1.5 to 4
- yield_stress: float32 [4], replicated, may hold values from 0.5 to 3
- accepted: int32 [1], replicated, may hold values from 0 to 3
Outputs:
- norms: float32 [2, 4], replicated
- chosen_velocity: float32 [3, 16, 32, 512], P(None, 'gx', 'gy', 'gz')
- chosen_residual: float32 [3, 16, 32, 512], P(None, 'gx', 'gy', 'gz')
The draws below stay inside these ranges and needn't reach their ends.
Inputs may be any that keep to these rules, and one draw needn't show every extreme that they name: `body_force`: body force on every cell and component.
All inputs are finite; a program needn't handle non-finite values.
Results may differ from the reference program's by a relative error of at most 0.00022.
Values sent between devices are 32-bit elements; how exact they have to be, the bound alone decides.
A program may use at most 64 MiB of HBM per device.

```python
import math
import jax
import jax.numpy as jnp
from jax import lax

NPHASE = 4
NX = 16
NY = 32
NZ = 512


def draw_body_force(key, part):
    xpos = jnp.arange(NX, dtype=jnp.float32) / NX
    ypos = jnp.arange(NY, dtype=jnp.float32) / NY
    zpos = jnp.arange(NZ, dtype=jnp.float32) / NZ
    growth = jnp.power(3.0, 0.5 * (xpos[:, None, None] + ypos[None, :, None] + zpos[None, None, :]))
    rough = jax.random.truncated_normal(jax.random.fold_in(key, 7), -4.0, 4.0, (3, NX, NY, NZ), jnp.float32)
    return rough * growth[None]


def place_ends(result, stream_key, smallest, top_value):
    longest = result.shape.index(max(result.shape))
    spots = []
    for shift in (0, 1):
        where = [jax.random.randint(jax.random.fold_in(stream_key, axis), (), 0, length) for axis, length in enumerate(result.shape)]
        where[longest] = (where[longest] + shift) % result.shape[longest]
        spots.append(tuple(where))
    return result.at[spots[0]].set(smallest).at[spots[1]].set(top_value)


def steps_of(rng, shape, shards, smallest, largest):
    factor_of = 1.0
    for axis_at, shards_of in shards:
        draws = jax.random.uniform(jax.random.fold_in(jax.random.fold_in(rng, 6), axis_at), (shards_of,), jnp.float32, smallest / len(shards), largest / len(shards))
        factor_of = factor_of * jnp.repeat(jnp.exp(draws), shape[axis_at] // shards_of).reshape((-1,) + (1,) * (len(shape) - 1 - axis_at))
    return factor_of


def bell_draw(own_key, extent, deviation, most, split=(), held_as=jnp.bfloat16):
    result = jax.random.normal(own_key, extent, jnp.float32) * deviation
    if len(split) > 0:
        result = steps_of(own_key, extent, split, -0.22, 0.18) * result
    return jnp.clip(result, min=-most, max=most).astype(held_as)


def setup_inputs(seed: int = 0) -> dict:
    key_of = jax.random.split(jax.random.key(seed), 10)
    velocity = bell_draw(key_of[0], (3, NX, NY, NZ), 1.0, 6.0, ((1, 2), (2, 4), (3, 4)), jnp.float32)
    direction = bell_draw(key_of[1], (3, NX, NY, NZ), 0.5, 3.0, ((1, 2), (2, 4), (3, 4)), jnp.float32)
    pressure = bell_draw(key_of[2], (NX, NY, NZ), 1.0, 6.0, ((0, 2), (1, 4), (2, 4)), jnp.float32)
    body_force = draw_body_force(jax.random.fold_in(key_of[9], 71), 0)
    phase_ids = place_ends(jax.random.randint(key_of[4], (NX, NY, NZ), 0, NPHASE), jax.random.fold_in(key_of[4], 1), 0, NPHASE - 1).astype(jnp.int32)
    creep_factor = jnp.clip(jnp.exp(jax.random.uniform(key_of[5], (NPHASE,), jnp.float32, math.log(0.5), math.log(2.0))), 0.5, 2.0)
    stress_exponent = jnp.clip(jax.random.uniform(key_of[6], (NPHASE,), jnp.float32, 1.5, 4.0), 1.5, 4.0)
    yield_stress = jnp.clip(jnp.exp(jax.random.uniform(key_of[7], (NPHASE,), jnp.float32, math.log(0.5), math.log(3.0))), 0.5, 3.0)
    accepted = jax.random.randint(key_of[8], (1,), 0, 4).astype(jnp.int32)
    return dict(velocity=velocity, direction=direction, pressure=pressure, body_force=body_force, phase_ids=phase_ids, creep_factor=creep_factor, stress_exponent=stress_exponent, yield_stress=yield_stress, accepted=accepted)


step_lengths = (1.0, 0.5, 0.25, 0.125)
rate_offset = 0.01
viscosity_least = 0.05
tiny_mean = 1e-06
tensor_slots = ((0, 3, 4), (3, 1, 5), (4, 5, 2))

def centered(values, axis_number):
    lower = [slice(1, -1)] * 3
    upper = [slice(1, -1)] * 3
    lower[axis_number] = slice(0, -2)
    upper[axis_number] = slice(2, None)
    leading = (slice(None),) * (values.ndim - 3)
    return 0.5 * (values[leading + tuple(upper)] - values[leading + tuple(lower)])

def component(values, i):
    return lax.index_in_dim(values, i, values.ndim - 4, keepdims=False)

def strain_rates(padded):
    gradients = [[centered(component(padded, i), j) for j in range(3)] for i in range(3)]
    return jnp.stack([gradients[0][0], gradients[1][1], gradients[2][2], 0.5 * (gradients[0][1] + gradients[1][0]), 0.5 * (gradients[0][2] + gradients[2][0]), 0.5 * (gradients[1][2] + gradients[2][1])], axis=-4)

def double_dot(first, second):
    diagonal = component(first, 0) * component(second, 0) + component(first, 1) * component(second, 1) + component(first, 2) * component(second, 2)
    offdiag = component(first, 3) * component(second, 3) + component(first, 4) * component(second, 4) + component(first, 5) * component(second, 5)
    return diagonal + 2.0 * offdiag

def effective_viscosity(rates, factor, exponent, yields):
    second = 0.5 * double_dot(rates, rates) + rate_offset
    creep_part = factor * jnp.power(second, (1.0 - exponent) / (2.0 * exponent))
    plastic = 0.5 * yields * lax.rsqrt(second)
    total_part = creep_part + plastic
    viscosity = creep_part * plastic / total_part + viscosity_least
    creep_slope = creep_part * (1.0 - exponent) / (2.0 * exponent * second)
    plastic_slope = -plastic / (2.0 * second)
    derivative = (plastic * plastic * creep_slope + creep_part * creep_part * plastic_slope) / (total_part * total_part)
    return (viscosity, derivative)

def spread_cells(values):
    return jnp.expand_dims(values, values.ndim - 3)

def divergence(padded):
    return jnp.stack([centered(component(padded, tensor_slots[i][0]), 0) + centered(component(padded, tensor_slots[i][1]), 1) + centered(component(padded, tensor_slots[i][2]), 2) for i in range(3)], axis=-4)

def tangent_stress(viscosity, derivative, rates, change):
    return 2.0 * spread_cells(viscosity) * change + 2.0 * spread_cells(derivative * double_dot(rates, change)) * rates

def phase_params(phase_ids, creep_factor, stress_exponent, yield_stress):
    choose = (phase_ids[None] == jnp.arange(creep_factor.shape[0], dtype=jnp.int32)[:, None, None, None]).astype(jnp.float32)
    return tuple((lax.optimization_barrier(jnp.sum(choose * entries[:, None, None, None], axis=0)) for entries in (creep_factor, stress_exponent, yield_stress)))

def pad_cells(values):
    return jnp.pad(values, [(0, 0)] * (values.ndim - 3) + [(1, 1)] * 3)

def reference(velocity, direction, pressure, body_force, phase_ids, creep_factor, stress_exponent, yield_stress, accepted):
    factor, exponent, yields = phase_params(phase_ids, creep_factor, stress_exponent, yield_stress)
    padded_pressure = pad_cells(pressure)
    loading = body_force - jnp.stack([centered(padded_pressure, j) for j in range(3)])
    base_rates = strain_rates(pad_cells(velocity))
    base_viscosity, base_slope = effective_viscosity(base_rates, factor, exponent, yields)
    residual_base = divergence(pad_cells(2.0 * spread_cells(base_viscosity) * base_rates)) + loading
    change_rates = strain_rates(pad_cells(direction))
    jacobian = divergence(pad_cells(tangent_stress(base_viscosity, base_slope, base_rates, change_rates)))
    cells = 3.0 * velocity.shape[1] * velocity.shape[2] * velocity.shape[3]
    actual = []
    predicted = []
    chosen_velocity = jnp.zeros_like(velocity)
    chosen_residual = jnp.zeros_like(velocity)
    for number, length in enumerate(step_lengths):
        trial_velocity = velocity + length * direction
        trial_rates = strain_rates(pad_cells(trial_velocity))
        trial_viscosity, unused_slope = effective_viscosity(trial_rates, factor, exponent, yields)
        trial_residual = divergence(pad_cells(2.0 * spread_cells(trial_viscosity) * trial_rates)) + loading
        linear = residual_base + length * jacobian
        actual.append(jnp.sum(trial_residual * trial_residual))
        predicted.append(jnp.sum(linear * linear))
        picked = accepted[0] == number
        chosen_velocity = jnp.where(picked, trial_velocity, chosen_velocity)
        chosen_residual = jnp.where(picked, trial_residual, chosen_residual)
    sums = jnp.stack(actual + predicted)
    norms = jnp.sqrt(sums / cells + tiny_mean).reshape(2, 4)
    return (norms, chosen_velocity, chosen_residual)
```

```python
import functools

import jax
import jax.numpy as jnp
from jax import lax
from jax.experimental import pallas as pl
from jax.experimental.pallas import tpu as pltpu
from jax.sharding import PartitionSpec as P

step_lengths = (1.0, 0.5, 0.25, 0.125)
rate_offset = 0.01
viscosity_least = 0.05
tiny_mean = 1e-06
MESH = pl.DeviceIdType.MESH
AXES = ("gx", "gy", "gz")
INV_LN2 = 1.4426950408889634
FACE_COMPONENTS = ((0, 3, 4), (3, 1, 5), (4, 5, 2))


def spin(values, shift, axis):
    return pltpu.roll(values, shift % values.shape[axis], axis)


def offsets():
    found = []
    for dx in (-1, 0, 1):
        for dy in (-1, 0, 1):
            for dz in (-1, 0, 1):
                if 1 <= abs(dx) + abs(dy) + abs(dz) <= 2:
                    found.append((dx, dy, dz))
    return sorted(found, key=lambda o: (o[2] != 0, sum(map(abs, o))))


def stress_fields(E, F, phase, params, components, mask):
    factors, powers, yields = params
    factor, power, half_yield = factors[-1], powers[-1], yields[-1]
    for k in range(len(factors) - 2, -1, -1):
        here = phase == float(k)
        factor = jnp.where(here, factors[k], factor)
        power = jnp.where(here, powers[k], power)
        half_yield = jnp.where(here, yields[k], half_yield)

    def dot(a, b):
        diagonal = a[0] * b[0] + a[1] * b[1] + a[2] * b[2]
        return diagonal + 2.0 * (a[3] * b[3] + a[4] * b[4] + a[5] * b[5])

    def parts(rates):
        second = 0.125 * dot(rates, rates) + rate_offset
        creep = factor * jnp.exp2(power * jnp.log(second))
        plastic = half_yield * lax.rsqrt(second)
        total = creep + plastic
        inverse = 1.0 / total
        return second, creep, plastic, inverse, creep * plastic * inverse

    second, creep, plastic, inverse, mixed = parts(E)
    half = 0.5 * mixed + 0.5 * viscosity_least
    slope = mixed * (plastic * (power * (1.0 / INV_LN2)) - 0.5 * creep) * inverse / second
    coupling = 0.125 * slope * dot(E, F)
    if mask is not None:
        half = half * mask
        coupling = coupling * mask
    fields = [[half * E[i] for i in components]]
    fields.append([half * F[i] + coupling * E[i] for i in components])
    for length in step_lengths:
        rates = [e + length * f if length != 1.0 else e + f for e, f in zip(E, F)]
        half = 0.5 * parts(rates)[4] + 0.5 * viscosity_least
        if mask is not None:
            half = half * mask
        fields.append([half * rates[i] for i in components])
    return fields


def twice_rates(g):
    return [
        g[0][0],
        g[1][1],
        g[2][2],
        0.5 * (g[0][1] + g[1][0]),
        0.5 * (g[0][2] + g[2][0]),
        0.5 * (g[1][2] + g[2][1]),
    ]


def kernel(
    sizes,
    creep_ref, exponent_ref, yield_ref, accepted_ref,
    v_ref, d_ref, p_ref, b_ref, m_ref,
    norms_ref, cv_ref, cr_ref,
    sx, sy, sxy, sz,
    rx, ry, rz, rxy, rxz, ryz,
    own, xs_ref, ys_ref, red,
    send_sem, recv_sem, red_send, red_recv,
):
    nx, ny, nz = v_ref.shape[1:]
    me = [lax.axis_index(a) for a in AXES]
    offs = offsets()

    def exists(o):
        ok = None
        for k in range(3):
            if o[k]:
                here = me[k] > 0 if o[k] < 0 else me[k] < sizes[k] - 1
                ok = here if ok is None else jnp.logical_and(ok, here)
        return ok

    def device(o):
        return tuple(me[k] + o[k] for k in range(3))

    def mate(axis, off):
        place = list(me)
        place[axis] = lax.rem(me[axis] + off, sizes[axis])
        return tuple(place)

    barrier = pltpu.get_barrier_semaphore()
    count = sum(n - 1 for n in sizes)
    for o in offs:
        @pl.when(exists(o))
        def _():
            pl.semaphore_signal(barrier, inc=1, device_id=device(o), device_id_type=MESH)
        count = count + exists(o).astype(jnp.int32)
    for axis in range(3):
        for off in range(1, sizes[axis]):
            pl.semaphore_signal(barrier, inc=1, device_id=mate(axis, off), device_id_type=MESH)

    sub = lax.broadcasted_iota(jnp.int32, (ny, nz), 0)
    lane = lax.broadcasted_iota(jnp.int32, (ny, nz), 1)
    quad = lane % 4
    first, last = lane == 0, lane == nz - 1
    top, bottom = sub == 0, sub == ny - 1
    is_left = quad < 2

    def vel(c, x):
        return v_ref[c, x] if c < 3 else d_ref[c - 3, x]

    def entity(e, x):
        if e < 6:
            return vel(e, x)
        return p_ref[x] if e == 6 else m_ref[x].astype(jnp.float32)

    for s in range(2):
        near, far = (0, 1) if s == 0 else (nx - 1, nx - 2)
        for c in range(6):
            sx[s, 2 * c] = vel(c, near)
            sx[s, 2 * c + 1] = vel(c, far)
        sx[s, 12] = p_ref[near]
        sx[s, 13] = m_ref[near].astype(jnp.float32)
        near, far = (0, 1) if s == 0 else (ny - 1, ny - 2)
        edge = jnp.zeros((nx, nz), jnp.float32)
        for c in range(6):
            source = v_ref if c < 3 else d_ref
            plane = source[c % 3, :, near, :]
            sy[s, 2 * c] = plane
            sy[s, 2 * c + 1] = source[c % 3, :, far, :]
            edge = jnp.where(lane // 2 == c, spin(plane, 2 * c + 1, 1), edge)
            for side in range(2):
                x = 0 if side == 0 else nx - 1
                sxy[side, s, pl.ds(c, 1), :] = source[c % 3, x, pl.ds(near, 1), :]
        sy[s, 12] = p_ref[:, near, :]
        sy[s, 13] = m_ref[:, near, :].astype(jnp.float32)
        sz[s, 2] = edge
    for half in range(2):
        pack = jnp.zeros((ny, nz), jnp.float32)
        for e in range(4):
            for x in range(nx):
                base = 4 * (e * nx + x)
                pack = jnp.where(lane // 4 == base // 4, spin(entity(4 * half + e, x), base + 2, 1), pack)
        sz[0, half] = pack
        sz[1, half] = pack

    def ends(o):
        side = [(k + 1) // 2 for k in o]
        back = [1 - k for k in side]
        dx, dy, dz = o
        if dx and dy:
            return sxy.at[side[0], side[1]], rxy.at[back[0], back[1]]
        if dx and dz:
            return sz.at[0, pl.ds(0, 2)], rxz.at[back[0], back[2]]
        if dy and dz:
            return sz.at[side[1]], ryz.at[back[1], back[2]]
        if dx:
            return sx.at[side[0]], rx.at[back[0]]
        if dy:
            return sy.at[side[1]], ry.at[back[1]]
        return sz.at[0, pl.ds(0, 2)], rz.at[back[2]]

    def copy_of(o):
        source, target = ends(o)
        mirror = tuple(-k for k in o)
        return pltpu.make_async_remote_copy(
            src_ref=source, dst_ref=target,
            send_sem=send_sem.at[offs.index(o)], recv_sem=recv_sem.at[offs.index(mirror)],
            device_id=device(o), device_id_type=MESH,
        )

    pl.semaphore_wait(barrier, count)
    for o in offs:
        @pl.when(exists(o))
        def _():
            copy_of(o).start()

    lengths = jnp.float32(step_lengths[-1])
    accepted = accepted_ref[0]
    for k in range(len(step_lengths) - 2, -1, -1):
        lengths = jnp.where(accepted == k, jnp.float32(step_lengths[k]), lengths)
    for c in range(3):
        for x in range(nx):
            cv_ref[c, x] = v_ref[c, x] + lengths * d_ref[c, x]

    phases = creep_ref.shape[0]
    full = lambda value: jnp.full((ny, nz), value, jnp.float32)
    factors = [full(creep_ref[k]) for k in range(phases)]
    halves = [0.5 * full(yield_ref[k]) for k in range(phases)]
    powers = []
    for k in range(phases):
        n = full(exponent_ref[k])
        powers.append((1.0 - n) / (2.0 * n) * INV_LN2)
    params = (factors, powers, halves)

    for o in offs:
        mirror = tuple(-k for k in o)
        _, target = ends(mirror)

        @pl.when(exists(o))
        def _():
            copy_of(mirror).wait_recv()

        @pl.when(jnp.logical_not(exists(o)))
        def _():
            target[...] = jnp.zeros(target.shape, jnp.float32)

    def along_y(V, before, after):
        down = spin(jnp.where(bottom, before, V), 1, 0)
        up = spin(jnp.where(top, after, V), -1, 0)
        return up - down

    def along_z(V, T):
        down = spin(jnp.where(last, T, V), 1, 1)
        up = spin(jnp.where(first, T, V), -1, 1)
        return up - down

    def scale_of(o):
        return jnp.full((ny, nz), exists(o).astype(jnp.float32))

    W = [jnp.where(is_left, rz[0, h], rz[1, h]) for h in range(2)]
    XW = [[jnp.where(is_left, rxz[s, 0, h], rxz[s, 1, h]) for h in range(2)] for s in range(2)]
    YW = [[jnp.where(is_left, ryz[s, 0, h], ryz[s, 1, h]) for h in range(2)] for s in range(2)]
    YE = [jnp.where(lane % 2 == 0, ryz[s, 0, 2], ryz[s, 1, 2]) for s in range(2)]

    def quad_at(packed, e, x):
        return spin(packed[e // 4], -(4 * ((e % 4) * nx + x) + 2), 1)

    for s in range(2):
        x = 0 if s == 0 else nx - 1
        g = []
        for c in range(6):
            B, A, O = rx[s, 2 * c], rx[s, 2 * c + 1], vel(c, x)
            dx = O - A if s == 0 else A - O
            dy = along_y(B, rxy[s, 0, pl.ds(c, 1), :], rxy[s, 1, pl.ds(c, 1), :])
            dz = along_z(B, quad_at(XW[s], c, nx - 1 - x))
            g.append((dx, dy, dz))
        fields = stress_fields(
            twice_rates(g[:3]), twice_rates(g[3:]), rx[s, 13], params,
            FACE_COMPONENTS[0], scale_of((2 * s - 1, 0, 0)),
        )
        for f in range(6):
            for i in range(3):
                xs_ref[s, 3 * f + i] = fields[f][i]

    for s in range(2):
        g = []
        for c in range(6):
            B, A, O = ry[s, 2 * c], ry[s, 2 * c + 1], sy[s, 2 * c]
            dy = O - A if s == 0 else A - O
            dx = along_y(B, rxy[0, s, pl.ds(c, 1), :], rxy[1, s, pl.ds(c, 1), :])
            dz = along_z(B, spin(YE[s], -(2 * c + 1), 1))
            g.append((dx, dy, dz))
        fields = stress_fields(
            twice_rates(g[:3]), twice_rates(g[3:]), ry[s, 13], params,
            FACE_COMPONENTS[1], scale_of((0, 2 * s - 1, 0)),
        )
        for f in range(6):
            for i in range(3):
                ys_ref[s, 3 * f + i] = fields[f][i]

    spot = (lane // 4) % nx
    packed = []
    for h in range(2):
        O = sz[0, h]
        dz = jnp.where(
            quad == 1,
            spin(O, -1, 1) - spin(W[h], 1, 1),
            spin(W[h], -1, 1) - spin(O, 1, 1),
        )
        turn = 4 * (nx - 1)
        down = jnp.where(spot == 0, spin(XW[0][h], -turn, 1), spin(W[h], 4, 1))
        up = jnp.where(spot == nx - 1, spin(XW[1][h], turn, 1), spin(W[h], -4, 1))
        dy = along_y(W[h], YW[0][h], YW[1][h])
        packed.append((up - down, dy, dz))
    g = []
    for c in range(6):
        g.append([spin(packed[c // 4][j], -4 * nx * (c % 4), 1) for j in range(3)])
    inside = jnp.where(
        quad == 1, scale_of((0, 0, -1)), jnp.where(quad == 2, scale_of((0, 0, 1)), 0.0)
    )
    z_fields = stress_fields(
        twice_rates(g[:3]), twice_rates(g[3:]), spin(W[1], -4 * nx * 3, 1), params,
        FACE_COMPONENTS[2], inside,
    )

    for x in range(nx):
        g = []
        for c in range(6):
            V = vel(c, x)
            after = vel(c, x + 1) if x < nx - 1 else rx[1, 2 * c]
            before = vel(c, x - 1) if x > 0 else rx[0, 2 * c]
            dy = along_y(V, ry[0, 2 * c, pl.ds(x, 1), :], ry[1, 2 * c, pl.ds(x, 1), :])
            g.append((after - before, dy, along_z(V, quad_at(W, c, x))))
        fields = stress_fields(
            twice_rates(g[:3]), twice_rates(g[3:]), m_ref[x].astype(jnp.float32), params,
            range(6), None,
        )
        for f in range(6):
            for i in range(6):
                own[6 * f + i, x] = fields[f][i]

    sums = [jnp.zeros((ny, nz), jnp.float32) for _ in range(8)]
    for x in range(nx):
        pressure = p_ref[x]
        after = p_ref[x + 1] if x < nx - 1 else rx[1, 12]
        before = p_ref[x - 1] if x > 0 else rx[0, 12]
        slopes = (
            after - before,
            along_y(pressure, ry[0, 12, pl.ds(x, 1), :], ry[1, 12, pl.ds(x, 1), :]),
            along_z(pressure, quad_at(W, 6, x)),
        )
        for i in range(3):
            a, b, c = (FACE_COMPONENTS[j][i] for j in range(3))
            loading = b_ref[i, x] - 0.5 * slopes[i]
            divided = []
            for f in range(6):
                after = own[6 * f + a, x + 1] if x < nx - 1 else xs_ref[1, 3 * f + i]
                before = own[6 * f + a, x - 1] if x > 0 else xs_ref[0, 3 * f + i]
                dy = along_y(
                    own[6 * f + b, x],
                    ys_ref[0, 3 * f + i, pl.ds(x, 1), :],
                    ys_ref[1, 3 * f + i, pl.ds(x, 1), :],
                )
                dz = along_z(own[6 * f + c, x], spin(z_fields[f][i], -(4 * x + 2), 1))
                divided.append((after - before) + dy + dz)
            base = divided[0] + loading
            chosen = None
            for k in range(3, -1, -1):
                residual = divided[2 + k] + loading
                linear = base + step_lengths[k] * divided[1]
                sums[k] = sums[k] + residual * residual
                sums[4 + k] = sums[4 + k] + linear * linear
                chosen = residual if chosen is None else jnp.where(accepted == k, residual, chosen)
            cr_ref[i, x] = chosen

    total = jnp.zeros((ny, nz), jnp.float32)
    for k in range(8):
        total = jnp.where(sub == k, jnp.sum(sums[k], axis=0, keepdims=True), total)
    start = 0
    for axis in (2, 1, 0):
        n = sizes[axis]
        red[start + me[axis]] = total

        def share(off, incoming):
            other = lax.rem(me[axis] + off, n)
            slot = start + (other if incoming else me[axis])
            return pltpu.make_async_remote_copy(
                src_ref=red.at[start + me[axis]], dst_ref=red.at[slot],
                send_sem=red_send.at[start + off], recv_sem=red_recv.at[slot],
                device_id=mate(axis, off), device_id_type=MESH,
            )

        for off in range(1, n):
            share(off, False).start()
        for off in range(1, n):
            share(off, True).wait_recv()
        total = red[start]
        for j in range(1, n):
            total = total + red[start + j]
        for off in range(1, n):
            share(off, False).wait_send()
        start += n
    cells = 3.0 * nx * ny * nz * sizes[0] * sizes[1] * sizes[2]
    root = jnp.sqrt(jnp.sum(total, axis=1, keepdims=True) / cells + tiny_mean)
    spread = jnp.where(lane == sub % 4, root, 0.0)
    upper = jnp.sum(jnp.where(sub < 4, spread, 0.0), axis=0, keepdims=True)
    lower = jnp.sum(jnp.where(sub < 4, 0.0, spread), axis=0, keepdims=True)
    norms_ref[...] = jnp.concatenate([upper, lower], axis=0)[:, :4]

    for o in offs:
        @pl.when(exists(o))
        def _():
            copy_of(o).wait_send()


def body(velocity, direction, pressure, body_force, phase_ids, creep, exponent, yields, accepted):
    sizes = tuple(lax.axis_size(a) for a in AXES)
    tile = velocity.shape[2:]
    vmem = pl.BlockSpec(memory_space=pltpu.VMEM)
    smem = pl.BlockSpec(memory_space=pltpu.SMEM)
    slots = sum(sizes)

    def scratch(*lead):
        return pltpu.VMEM(lead + tile, jnp.float32)

    return pl.pallas_call(
        functools.partial(kernel, sizes),
        out_shape=(
            jax.ShapeDtypeStruct((2, 4), jnp.float32),
            jax.ShapeDtypeStruct(velocity.shape, jnp.float32),
            jax.ShapeDtypeStruct(velocity.shape, jnp.float32),
        ),
        in_specs=[smem] * 4 + [vmem] * 5,
        out_specs=(vmem, vmem, vmem),
        scratch_shapes=[
            scratch(2, 14), scratch(2, 14), scratch(2, 2), scratch(2, 3),
            scratch(2, 14), scratch(2, 14), scratch(2, 2), scratch(2, 2),
            scratch(2, 2, 2), scratch(2, 2, 3),
            scratch(36, velocity.shape[1]), scratch(2, 18), scratch(2, 18), scratch(slots),
            pltpu.SemaphoreType.DMA((18,)), pltpu.SemaphoreType.DMA((18,)),
            pltpu.SemaphoreType.DMA((slots,)), pltpu.SemaphoreType.DMA((slots,)),
        ],
        compiler_params=pltpu.CompilerParams(collective_id=0, has_side_effects=True),
    )(creep, exponent, yields, accepted, velocity, direction, pressure, body_force, phase_ids)


def solution(mesh):
    placed = (
        P(None, "gx", "gy", "gz"),
        P(None, "gx", "gy", "gz"),
        P("gx", "gy", "gz"),
        P(None, "gx", "gy", "gz"),
        P("gx", "gy", "gz"),
        P(),
        P(),
        P(),
        P(),
    )
    return jax.shard_map(
        body,
        mesh=mesh,
        in_specs=placed,
        out_specs=(P(), P(None, "gx", "gy", "gz"), P(None, "gx", "gy", "gz")),
        check_vma=False,
    )
```

```python
import functools

import jax
import jax.numpy as jnp
from jax import lax
from jax.experimental import pallas as pl
from jax.experimental.pallas import tpu as pltpu
from jax.sharding import PartitionSpec as P

step_lengths = (1.0, 0.5, 0.25, 0.125)
rate_offset = 0.01
viscosity_least = 0.05
tiny_mean = 1e-06
MESH = pl.DeviceIdType.MESH
AXES = ("gx", "gy", "gz")
INV_LN2 = 1.4426950408889634
FACE_COMPONENTS = ((0, 3, 4), (3, 1, 5), (4, 5, 2))


def spin(values, shift, axis):
    return pltpu.roll(values, shift % values.shape[axis], axis)


def offsets():
    found = []
    for dx in (-1, 0, 1):
        for dy in (-1, 0, 1):
            for dz in (-1, 0, 1):
                if 1 <= abs(dx) + abs(dy) + abs(dz) <= 2:
                    found.append((dx, dy, dz))
    return sorted(found, key=lambda o: (o[2] != 0, sum(map(abs, o))))


def stress_fields(E, F, phase, params, components, mask):
    factors, powers, yields = params
    factor, power, half_yield = factors[-1], powers[-1], yields[-1]
    for k in range(len(factors) - 2, -1, -1):
        here = phase == float(k)
        factor = jnp.where(here, factors[k], factor)
        power = jnp.where(here, powers[k], power)
        half_yield = jnp.where(here, yields[k], half_yield)

    def dot(a, b):
        diagonal = a[0] * b[0] + a[1] * b[1] + a[2] * b[2]
        return diagonal + 2.0 * (a[3] * b[3] + a[4] * b[4] + a[5] * b[5])

    def parts(rates):
        second = 0.125 * dot(rates, rates) + rate_offset
        creep = factor * jnp.exp2(power * jnp.log(second))
        plastic = half_yield * lax.rsqrt(second)
        total = creep + plastic
        inverse = 1.0 / total
        return second, creep, plastic, inverse, creep * plastic * inverse

    second, creep, plastic, inverse, mixed = parts(E)
    half = 0.5 * mixed + 0.5 * viscosity_least
    slope = mixed * (plastic * (power * (1.0 / INV_LN2)) - 0.5 * creep) * inverse / second
    coupling = 0.125 * slope * dot(E, F)
    if mask is not None:
        half = half * mask
        coupling = coupling * mask
    fields = [[half * E[i] for i in components]]
    fields.append([half * F[i] + coupling * E[i] for i in components])
    for length in step_lengths:
        rates = [e + length * f if length != 1.0 else e + f for e, f in zip(E, F)]
        half = 0.5 * parts(rates)[4] + 0.5 * viscosity_least
        if mask is not None:
            half = half * mask
        fields.append([half * rates[i] for i in components])
    return fields


def twice_rates(g):
    return [
        g[0][0],
        g[1][1],
        g[2][2],
        0.5 * (g[0][1] + g[1][0]),
        0.5 * (g[0][2] + g[2][0]),
        0.5 * (g[1][2] + g[2][1]),
    ]


def kernel(
    sizes,
    creep_ref, exponent_ref, yield_ref, accepted_ref,
    v_hbm, d_hbm, p_hbm, b_hbm, m_hbm,
    norms_ref, cv_ref, cr_ref,
    vx, px, mx, bx, sy, sxy, sz, ry, yr, rz, rxz, ryz,
    w3, grads, stress, phases, masks, red,
    load_sem, send_sem, recv_sem, red_send, red_recv,
):
    nx, ny, nz = v_hbm.shape[1:]
    me = [lax.axis_index(a) for a in AXES]
    devices = sizes[0] * sizes[1] * sizes[2]
    rank = (me[0] * sizes[1] + me[1]) * sizes[2] + me[2]
    offs = offsets()

    loads = [
        pltpu.make_async_copy(source, target, load_sem.at[n])
        for n, (source, target) in enumerate((
            (v_hbm, vx.at[pl.ds(0, 3), pl.ds(2, nx)]),
            (d_hbm, vx.at[pl.ds(3, 3), pl.ds(2, nx)]),
            (p_hbm, px.at[pl.ds(1, nx)]),
            (m_hbm, mx.at[pl.ds(1, nx)]),
            (b_hbm, bx),
        ))
    ]
    for load in loads:
        load.start()

    def mate(k):
        other = lax.rem(rank + k, devices)
        return (
            other // (sizes[1] * sizes[2]),
            lax.rem(other // sizes[2], sizes[1]),
            lax.rem(other, sizes[2]),
        )

    barrier = pltpu.get_barrier_semaphore()

    def greet(k, carry):
        pl.semaphore_signal(barrier, inc=1, device_id=mate(k), device_id_type=MESH)
        return carry

    lax.fori_loop(1, devices, greet, 0)

    inner = [(me[k] > 0, me[k] < sizes[k] - 1) for k in range(3)]

    def exists(o):
        ok = None
        for k in range(3):
            if o[k]:
                here = inner[k][(o[k] + 1) // 2]
                ok = here if ok is None else jnp.logical_and(ok, here)
        return ok

    def device(o):
        return tuple(me[k] + o[k] for k in range(3))

    sub = lax.broadcasted_iota(jnp.int32, (ny, nz), 0)
    lane = lax.broadcasted_iota(jnp.int32, (ny, nz), 1)
    quad = lane % 4
    first, last = lane == 0, lane == nz - 1
    top, bottom = sub == 0, sub == ny - 1
    is_left = quad < 2

    for load in loads[:4]:
        load.wait()

    def gather(x, packs):
        packs = list(packs)
        for e in range(8):
            if e < 6:
                plane = vx[e, x + 2]
            else:
                plane = px[x + 1] if e == 6 else mx[x + 1].astype(jnp.float32)
            base = 4 * ((e % 4) * nx + x)
            turned = pltpu.roll(plane, lax.rem(base + 2, nz), 1)
            packs[e // 4] = jnp.where(lane // 4 == base // 4, turned, packs[e // 4])
        for s in range(2):
            near, far = (0, 1) if s == 0 else (ny - 1, ny - 2)
            for c in range(6):
                sy[s, 2 * c, pl.ds(x, 1), :] = vx[c, x + 2, pl.ds(near, 1), :]
                sy[s, 2 * c + 1, pl.ds(x, 1), :] = vx[c, x + 2, pl.ds(far, 1), :]
            sy[s, 12, pl.ds(x, 1), :] = px[x + 1, pl.ds(near, 1), :]
            sy[s, 13, pl.ds(x, 1), :] = mx[x + 1, pl.ds(near, 1), :].astype(jnp.float32)
        return tuple(packs)

    blank = jnp.zeros((ny, nz), jnp.float32)
    packs = lax.fori_loop(0, nx, gather, (blank, blank))
    for s in range(2):
        near = 0 if s == 0 else ny - 1
        edge = blank
        for c in range(6):
            edge = jnp.where(lane // 2 == c, spin(sy[s, 2 * c], 2 * c + 1, 1), edge)
            for side in range(2):
                sxy[side, s, c] = vx[c, 2 + side * (nx - 1), pl.ds(near, 1), :]
        sz[s, 0] = packs[0]
        sz[s, 1] = packs[1]
        sz[s, 2] = edge

    def ends(o):
        side = [(k + 1) // 2 for k in o]
        back = [1 - k for k in side]
        dx, dy, dz = o
        if dx and dy:
            return [(sxy.at[side[0], side[1]], yr.at[back[1], back[0] * (nx + 1), pl.ds(0, 6)])]
        if dx and dz:
            return [(sz.at[0, pl.ds(0, 2)], rxz.at[back[0], back[2]])]
        if dy and dz:
            return [(sz.at[side[1]], ryz.at[back[1], back[2]])]
        if dx:
            mine, theirs = (2, nx + 2) if dx < 0 else (nx, 0)
            one, other = (1, nx + 1) if dx < 0 else (nx, 0)
            return [
                (vx.at[:, pl.ds(mine, 2)], vx.at[:, pl.ds(theirs, 2)]),
                (px.at[one], px.at[other]),
                (mx.at[one], mx.at[other]),
            ]
        if dy:
            return [(sy.at[side[1]], ry.at[back[1]])]
        return [(sz.at[0, pl.ds(0, 2)], rz.at[back[2]])]

    def copies_of(o):
        mirror = tuple(-k for k in o)
        return [
            pltpu.make_async_remote_copy(
                src_ref=source, dst_ref=target,
                send_sem=send_sem.at[offs.index(o), n], recv_sem=recv_sem.at[offs.index(mirror), n],
                device_id=device(o), device_id_type=MESH,
            )
            for n, (source, target) in enumerate(ends(o))
        ]

    pl.semaphore_wait(barrier, devices - 1)
    for o in offs:
        @pl.when(exists(o))
        def _():
            for copy in copies_of(o):
                copy.start()

    accepted = accepted_ref[0]
    length = jnp.float32(step_lengths[-1])
    for k in range(len(step_lengths) - 2, -1, -1):
        length = jnp.where(accepted == k, jnp.float32(step_lengths[k]), length)

    def ahead(x, carry):
        for c in range(3):
            cv_ref[c, x] = vx[c, x + 2] + length * vx[c + 3, x + 2]
        phases[x + 1] = mx[x + 1].astype(jnp.float32)
        masks[x + 1] = jnp.ones((ny, nz), jnp.float32)
        return carry

    lax.fori_loop(0, nx, ahead, 0)

    full = lambda value: jnp.full((ny, nz), value, jnp.float32)
    count = creep_ref.shape[0]
    factors = [full(creep_ref[k]) for k in range(count)]
    halves = [0.5 * full(yield_ref[k]) for k in range(count)]
    powers = []
    for k in range(count):
        n = full(exponent_ref[k])
        powers.append((1.0 - n) / (2.0 * n) * INV_LN2)
    params = (factors, powers, halves)

    def scale_of(o):
        return jnp.full((ny, nz), exists(o).astype(jnp.float32))

    for s in range(2):
        masks[s * (nx + 1)] = scale_of((2 * s - 1, 0, 0))
        masks[nx + 2 + s] = scale_of((0, 2 * s - 1, 0))
    masks[nx + 4] = jnp.where(
        quad == 1, scale_of((0, 0, -1)), jnp.where(quad == 2, scale_of((0, 0, 1)), 0.0)
    )

    for o in offs:
        mirror = tuple(-k for k in o)

        @pl.when(exists(o))
        def _():
            for copy in copies_of(mirror):
                copy.wait_recv()

        @pl.when(jnp.logical_not(exists(o)))
        def _():
            for _, target in ends(mirror):
                target[...] = jnp.zeros(target.shape, target.dtype)

    def along_y(V, before, after):
        down = spin(jnp.where(bottom, before, V), 1, 0)
        up = spin(jnp.where(top, after, V), -1, 0)
        return up - down

    def along_z(V, T):
        down = spin(jnp.where(last, T, V), 1, 1)
        up = spin(jnp.where(first, T, V), -1, 1)
        return up - down

    for h in range(2):
        w3[1, h] = jnp.where(is_left, rz[0, h], rz[1, h])
        for s in range(2):
            w3[2 * s, h] = jnp.where(is_left, rxz[s, 0, h], rxz[s, 1, h])

    def rows(x, carry):
        for s in range(2):
            for c in range(7):
                yr[s, x + 1, c] = ry[s, 2 * c, pl.ds(x, 1), :]
        return carry

    lax.fori_loop(0, nx, rows, 0)
    for s in range(2):
        phases[s * (nx + 1)] = mx[s * (nx + 1)].astype(jnp.float32)
        phases[nx + 2 + s] = ry[s, 13]

    def inside(q, carry):
        third = jnp.where(q == 0, 0, jnp.where(q == nx + 1, 2, 1))
        x = lax.rem(q + nx - 1, nx)
        for c in range(6):
            V = vx[c, q + 1]
            T = pltpu.roll(w3[third, c // 4], nz - (4 * ((c % 4) * nx + x) + 2), 1)
            grads[3 * c, q] = vx[c, q + 2] - vx[c, q]
            grads[3 * c + 1, q] = along_y(V, yr[0, q, c], yr[1, q, c])
            grads[3 * c + 2, q] = along_z(V, T)
        return carry

    lax.fori_loop(0, nx + 2, inside, 0)

    def sides(s, carry):
        sign = jnp.where(s == 0, jnp.float32(1.0), jnp.float32(-1.0))
        E = jnp.where(lane % 2 == 0, ryz[s, 0, 2], ryz[s, 1, 2])
        for c in range(6):
            B = ry[s, 2 * c]
            grads[3 * c, nx + 2 + s] = along_y(B, yr[s, 0, c], yr[s, nx + 1, c])
            grads[3 * c + 1, nx + 2 + s] = sign * (sy[s, 2 * c] - ry[s, 2 * c + 1])
            grads[3 * c + 2, nx + 2 + s] = along_z(B, spin(E, -(2 * c + 1), 1))
        return carry

    lax.fori_loop(0, 2, sides, 0)

    spot = (lane // 4) % nx
    turn = 4 * (nx - 1)
    for h in range(2):
        O, W = sz[0, h], w3[1, h]
        dz = jnp.where(quad == 1, spin(O, -1, 1) - spin(W, 1, 1), spin(W, -1, 1) - spin(O, 1, 1))
        down = jnp.where(spot == 0, spin(w3[0, h], -turn, 1), spin(W, 4, 1))
        up = jnp.where(spot == nx - 1, spin(w3[2, h], turn, 1), spin(W, -4, 1))
        before = jnp.where(is_left, ryz[0, 0, h], ryz[0, 1, h])
        after = jnp.where(is_left, ryz[1, 0, h], ryz[1, 1, h])
        packed = (up - down, along_y(W, before, after), dz)
        for c in range(4 * h, min(4 * h + 4, 6)):
            for j in range(3):
                grads[3 * c + j, nx + 4] = spin(packed[j], -4 * nx * (c % 4), 1)
    phases[nx + 4] = spin(w3[1, 1], -4 * nx * 3, 1)

    def stresses(q, carry):
        g = [[grads[3 * c + j, q] for j in range(3)] for c in range(6)]
        fields = stress_fields(
            twice_rates(g[:3]), twice_rates(g[3:]), phases[q], params, range(6), masks[q]
        )
        for f in range(6):
            for i in range(6):
                stress[6 * f + i, q] = fields[f][i]
        return carry

    lax.fori_loop(0, nx + 5, stresses, 0)
    loads[4].wait()

    def residuals(x, sums):
        sums = list(sums)
        turn = nz - (4 * x + 2)
        T = pltpu.roll(w3[1, 1], nz - (4 * (2 * nx + x) + 2), 1)
        slopes = (
            px[x + 2] - px[x],
            along_y(px[x + 1], yr[0, x + 1, 6], yr[1, x + 1, 6]),
            along_z(px[x + 1], T),
        )
        for i in range(3):
            a, b, c = (FACE_COMPONENTS[j][i] for j in range(3))
            loading = bx[i, x] - 0.5 * slopes[i]
            divided = []
            for f in range(6):
                dx = stress[6 * f + a, x + 2] - stress[6 * f + a, x]
                dy = along_y(
                    stress[6 * f + b, x + 1],
                    stress[6 * f + b, nx + 2, pl.ds(x, 1), :],
                    stress[6 * f + b, nx + 3, pl.ds(x, 1), :],
                )
                dz = along_z(stress[6 * f + c, x + 1], pltpu.roll(stress[6 * f + c, nx + 4], turn, 1))
                divided.append(dx + dy + dz)
            base = divided[0] + loading
            chosen = None
            for k in range(3, -1, -1):
                residual = divided[2 + k] + loading
                linear = base + step_lengths[k] * divided[1]
                sums[k] = sums[k] + residual * residual
                sums[4 + k] = sums[4 + k] + linear * linear
                chosen = residual if chosen is None else jnp.where(accepted == k, residual, chosen)
            cr_ref[i, x] = chosen
        return tuple(sums)

    sums = lax.fori_loop(0, nx, residuals, (blank,) * 8)

    total = blank
    for k in range(8):
        total = jnp.where(sub == k, jnp.sum(sums[k], axis=0, keepdims=True), total)
    total = jnp.sum(total, axis=1, keepdims=True)
    red[rank] = jnp.sum(jnp.where(lane == sub, total, 0.0), axis=0, keepdims=True)

    def share(k, carry):
        pltpu.make_async_remote_copy(
            src_ref=red.at[rank], dst_ref=red.at[rank], send_sem=red_send, recv_sem=red_recv,
            device_id=mate(k), device_id_type=MESH,
        ).start()
        return carry

    lax.fori_loop(1, devices, share, 0)
    others = red.at[pl.ds(0, devices - 1)]
    pltpu.make_async_copy(others, others, red_recv).wait()
    total = jnp.sum(red[...], axis=0)
    cells = 3.0 * nx * ny * nz * devices
    root = jnp.sqrt(total / cells + tiny_mean)
    norms_ref[0:1, :] = root[:, :4]
    norms_ref[1:2, :] = spin(jnp.broadcast_to(root, (ny, nz)), -4, 1)[0:1, :4]

    pltpu.make_async_copy(others, others, red_send).wait()
    for o in offs:
        @pl.when(exists(o))
        def _():
            for copy in copies_of(o):
                copy.wait_send()


def body(velocity, direction, pressure, body_force, phase_ids, creep, exponent, yields, accepted):
    sizes = tuple(lax.axis_size(a) for a in AXES)
    nx = velocity.shape[1]
    tile = velocity.shape[2:]
    row = (1, tile[1])
    vmem = pl.BlockSpec(memory_space=pltpu.VMEM)
    smem = pl.BlockSpec(memory_space=pltpu.SMEM)
    hbm = pl.BlockSpec(memory_space=pl.ANY)

    def scratch(*lead, held=jnp.float32, shape=tile):
        return pltpu.VMEM(lead + shape, held)

    return pl.pallas_call(
        functools.partial(kernel, sizes),
        out_shape=(
            jax.ShapeDtypeStruct((2, 4), jnp.float32),
            jax.ShapeDtypeStruct(velocity.shape, jnp.float32),
            jax.ShapeDtypeStruct(velocity.shape, jnp.float32),
        ),
        in_specs=[smem] * 4 + [hbm] * 5,
        out_specs=(vmem, vmem, vmem),
        scratch_shapes=[
            scratch(6, nx + 4), scratch(nx + 2), scratch(nx + 2, held=jnp.int32), scratch(3, nx),
            scratch(2, 14), scratch(2, 2, 6, shape=row), scratch(2, 3),
            scratch(2, 14), scratch(2, nx + 2, 7, shape=row), scratch(2, 2),
            scratch(2, 2, 2), scratch(2, 2, 3),
            scratch(3, 2), scratch(18, nx + 5), scratch(36, nx + 5), scratch(nx + 5), scratch(nx + 5),
            scratch(sizes[0] * sizes[1] * sizes[2], shape=row),
            pltpu.SemaphoreType.DMA((5,)),
            pltpu.SemaphoreType.DMA((18, 3)), pltpu.SemaphoreType.DMA((18, 3)),
            pltpu.SemaphoreType.DMA, pltpu.SemaphoreType.DMA,
        ],
        compiler_params=pltpu.CompilerParams(collective_id=0, has_side_effects=True),
    )(creep, exponent, yields, accepted, velocity, direction, pressure, body_force, phase_ids)


def solution(mesh):
    placed = (
        P(None, "gx", "gy", "gz"),
        P(None, "gx", "gy", "gz"),
        P("gx", "gy", "gz"),
        P(None, "gx", "gy", "gz"),
        P("gx", "gy", "gz"),
        P(),
        P(),
        P(),
        P(),
    )
    return jax.shard_map(
        body,
        mesh=mesh,
        in_specs=placed,
        out_specs=(P(), P(None, "gx", "gy", "gz"), P(None, "gx", "gy", "gz")),
        check_vma=False,
    )
```

```python
import functools

import jax
import jax.numpy as jnp
from jax import lax
from jax.experimental import pallas as pl
from jax.experimental.pallas import tpu as pltpu
from jax.sharding import PartitionSpec as P

step_lengths = (1.0, 0.5, 0.25, 0.125)
rate_offset = 0.01
viscosity_least = 0.05
tiny_mean = 1e-06
MESH = pl.DeviceIdType.MESH
AXES = ("gx", "gy", "gz")
INV_LN2 = 1.4426950408889634
FACE_COMPONENTS = ((0, 3, 4), (3, 1, 5), (4, 5, 2))


def spin(values, shift, axis):
    return pltpu.roll(values, shift % values.shape[axis], axis)


def offsets():
    found = []
    for dx in (-1, 0, 1):
        for dy in (-1, 0, 1):
            for dz in (-1, 0, 1):
                if 1 <= abs(dx) + abs(dy) + abs(dz) <= 2:
                    found.append((dx, dy, dz))
    return sorted(found, key=lambda o: (-sum(map(abs, o)), o[2] == 0))


def stress_fields(E, F, phase, params, components, mask):
    factors, powers, yields = params
    factor, power, half_yield = factors[-1], powers[-1], yields[-1]
    for k in range(len(factors) - 2, -1, -1):
        here = phase == float(k)
        factor = jnp.where(here, factors[k], factor)
        power = jnp.where(here, powers[k], power)
        half_yield = jnp.where(here, yields[k], half_yield)

    def dot(a, b):
        diagonal = a[0] * b[0] + a[1] * b[1] + a[2] * b[2]
        return diagonal + 2.0 * (a[3] * b[3] + a[4] * b[4] + a[5] * b[5])

    def parts(rates):
        second = 0.125 * dot(rates, rates) + rate_offset
        creep = factor * jnp.exp2(power * jnp.log(second))
        plastic = half_yield * lax.rsqrt(second)
        total = creep + plastic
        inverse = 1.0 / total
        return second, creep, plastic, inverse, creep * plastic * inverse

    second, creep, plastic, inverse, mixed = parts(E)
    half = 0.5 * mixed + 0.5 * viscosity_least
    slope = mixed * (plastic * (power * (1.0 / INV_LN2)) - 0.5 * creep) * inverse / second
    coupling = 0.125 * slope * dot(E, F)
    if mask is not None:
        half = half * mask
        coupling = coupling * mask
    fields = [[half * E[i] for i in components]]
    fields.append([half * F[i] + coupling * E[i] for i in components])
    for length in step_lengths:
        rates = [e + length * f if length != 1.0 else e + f for e, f in zip(E, F)]
        half = 0.5 * parts(rates)[4] + 0.5 * viscosity_least
        if mask is not None:
            half = half * mask
        fields.append([half * rates[i] for i in components])
    return fields


def twice_rates(g):
    return [
        g[0][0],
        g[1][1],
        g[2][2],
        0.5 * (g[0][1] + g[1][0]),
        0.5 * (g[0][2] + g[2][0]),
        0.5 * (g[1][2] + g[2][1]),
    ]


def kernel(
    sizes,
    creep_ref, exponent_ref, yield_ref, accepted_ref,
    v_hbm, d_hbm, p_hbm, b_hbm, m_hbm,
    norms_ref, cr_hbm,
    cr_ref, vx, px, mx, bx, sy, sxy, sz, ry, yr, rz, rxz, ryz,
    w3, grads, stress, phases, masks, red,
    load_sem, out_sem, send_sem, recv_sem, red_send, red_recv,
):
    nx, ny, nz = v_hbm.shape[1:]
    me = [lax.axis_index(a) for a in AXES]
    devices = sizes[0] * sizes[1] * sizes[2]
    rank = (me[0] * sizes[1] + me[1]) * sizes[2] + me[2]
    offs = offsets()

    loads = [
        pltpu.make_async_copy(source, target, load_sem.at[n])
        for n, (source, target) in enumerate((
            (v_hbm, vx.at[pl.ds(0, 3), pl.ds(2, nx)]),
            (d_hbm, vx.at[pl.ds(3, 3), pl.ds(2, nx)]),
            (p_hbm, px.at[pl.ds(1, nx)]),
            (m_hbm, mx.at[pl.ds(1, nx)]),
            (b_hbm, bx),
        ))
    ]
    for load in loads:
        load.start()

    def mate(k):
        other = lax.rem(rank + k, devices)
        return (
            other // (sizes[1] * sizes[2]),
            lax.rem(other // sizes[2], sizes[1]),
            lax.rem(other, sizes[2]),
        )

    barrier = pltpu.get_barrier_semaphore()

    def greet(k, carry):
        pl.semaphore_signal(barrier, inc=1, device_id=mate(k), device_id_type=MESH)
        return carry

    lax.fori_loop(1, devices, greet, 0)

    inner = [(me[k] > 0, me[k] < sizes[k] - 1) for k in range(3)]

    def exists(o):
        ok = None
        for k in range(3):
            if o[k]:
                here = inner[k][(o[k] + 1) // 2]
                ok = here if ok is None else jnp.logical_and(ok, here)
        return ok

    def device(o):
        return tuple(me[k] + o[k] for k in range(3))

    sub = lax.broadcasted_iota(jnp.int32, (ny, nz), 0)
    lane = lax.broadcasted_iota(jnp.int32, (ny, nz), 1)
    quad = lane % 4
    first, last = lane == 0, lane == nz - 1
    top, bottom = sub == 0, sub == ny - 1
    is_left = quad < 2

    for load in loads[:4]:
        load.wait()

    def gather(x, packs):
        packs = list(packs)
        for e in range(8):
            if e < 6:
                plane = vx[e, x + 2]
            else:
                plane = px[x + 1] if e == 6 else mx[x + 1].astype(jnp.float32)
            base = 4 * ((e % 4) * nx + x)
            turned = pltpu.roll(plane, lax.rem(base + 2, nz), 1)
            packs[e // 4] = jnp.where(lane // 4 == base // 4, turned, packs[e // 4])
        for s in range(2):
            near, far = (0, 1) if s == 0 else (ny - 1, ny - 2)
            for c in range(6):
                sy[s, 2 * c, pl.ds(x, 1), :] = vx[c, x + 2, pl.ds(near, 1), :]
                sy[s, 2 * c + 1, pl.ds(x, 1), :] = vx[c, x + 2, pl.ds(far, 1), :]
            sy[s, 12, pl.ds(x, 1), :] = px[x + 1, pl.ds(near, 1), :]
            sy[s, 13, pl.ds(x, 1), :] = mx[x + 1, pl.ds(near, 1), :].astype(jnp.float32)
        return tuple(packs)

    blank = jnp.zeros((ny, nz), jnp.float32)
    packs = lax.fori_loop(0, nx, gather, (blank, blank))
    for s in range(2):
        near = 0 if s == 0 else ny - 1
        edge = blank
        for c in range(6):
            edge = jnp.where(lane // 2 == c, spin(sy[s, 2 * c], 2 * c + 1, 1), edge)
            for side in range(2):
                sxy[side, s, c] = vx[c, 2 + side * (nx - 1), pl.ds(near, 1), :]
        sz[s, 0] = packs[0]
        sz[s, 1] = packs[1]
        sz[s, 2] = edge

    def ends(o):
        side = [(k + 1) // 2 for k in o]
        back = [1 - k for k in side]
        dx, dy, dz = o
        if dx and dy:
            return [(sxy.at[side[0], side[1]], yr.at[back[1], back[0] * (nx + 1), pl.ds(0, 6)])]
        if dx and dz:
            return [(sz.at[0, pl.ds(0, 2)], rxz.at[back[0], back[2]])]
        if dy and dz:
            return [(sz.at[side[1]], ryz.at[back[1], back[2]])]
        if dx:
            mine, theirs = (2, nx + 2) if dx < 0 else (nx, 0)
            one, other = (1, nx + 1) if dx < 0 else (nx, 0)
            return [
                (vx.at[:, pl.ds(mine, 2)], vx.at[:, pl.ds(theirs, 2)]),
                (px.at[one], px.at[other]),
                (mx.at[one], mx.at[other]),
            ]
        if dy:
            return [(sy.at[side[1]], ry.at[back[1]])]
        return [(sz.at[0, pl.ds(0, 2)], rz.at[back[2]])]

    def copies_of(o):
        mirror = tuple(-k for k in o)
        return [
            pltpu.make_async_remote_copy(
                src_ref=source, dst_ref=target,
                send_sem=send_sem.at[offs.index(o), n], recv_sem=recv_sem.at[offs.index(mirror), n],
                device_id=device(o), device_id_type=MESH,
            )
            for n, (source, target) in enumerate(ends(o))
        ]

    pl.semaphore_wait(barrier, devices - 1)
    for o in offs:
        @pl.when(exists(o))
        def _():
            for copy in copies_of(o):
                copy.start()

    accepted = accepted_ref[0]

    def ahead(x, carry):
        phases[x + 1] = mx[x + 1].astype(jnp.float32)
        masks[x + 1] = jnp.ones((ny, nz), jnp.float32)
        return carry

    lax.fori_loop(0, nx, ahead, 0)
    cr_out = pltpu.make_async_copy(cr_ref, cr_hbm, out_sem)

    full = lambda value: jnp.full((ny, nz), value, jnp.float32)
    count = creep_ref.shape[0]
    factors = [full(creep_ref[k]) for k in range(count)]
    halves = [0.5 * full(yield_ref[k]) for k in range(count)]
    powers = []
    for k in range(count):
        n = full(exponent_ref[k])
        powers.append((1.0 - n) / (2.0 * n) * INV_LN2)
    params = (factors, powers, halves)

    def scale_of(o):
        return jnp.full((ny, nz), exists(o).astype(jnp.float32))

    for s in range(2):
        masks[s * (nx + 1)] = scale_of((2 * s - 1, 0, 0))
        masks[nx + 2 + s] = scale_of((0, 2 * s - 1, 0))
    masks[nx + 4] = jnp.where(
        quad == 1, scale_of((0, 0, -1)), jnp.where(quad == 2, scale_of((0, 0, 1)), 0.0)
    )

    for o in offs:
        mirror = tuple(-k for k in o)

        @pl.when(exists(o))
        def _():
            for copy in copies_of(mirror):
                copy.wait_recv()

        @pl.when(jnp.logical_not(exists(o)))
        def _():
            for _, target in ends(mirror):
                target[...] = jnp.zeros(target.shape, target.dtype)

    def along_y(V, before, after):
        down = spin(jnp.where(bottom, before, V), 1, 0)
        up = spin(jnp.where(top, after, V), -1, 0)
        return up - down

    def along_z(V, T):
        down = spin(jnp.where(last, T, V), 1, 1)
        up = spin(jnp.where(first, T, V), -1, 1)
        return up - down

    for h in range(2):
        w3[1, h] = jnp.where(is_left, rz[0, h], rz[1, h])
        for s in range(2):
            w3[2 * s, h] = jnp.where(is_left, rxz[s, 0, h], rxz[s, 1, h])

    def rows(x, carry):
        for s in range(2):
            for c in range(7):
                yr[s, x + 1, c] = ry[s, 2 * c, pl.ds(x, 1), :]
        return carry

    lax.fori_loop(0, nx, rows, 0)
    for s in range(2):
        phases[s * (nx + 1)] = mx[s * (nx + 1)].astype(jnp.float32)
        phases[nx + 2 + s] = ry[s, 13]

    def inside(q, carry):
        third = jnp.where(q == 0, 0, jnp.where(q == nx + 1, 2, 1))
        x = lax.rem(q + nx - 1, nx)
        for c in range(6):
            V = vx[c, q + 1]
            T = pltpu.roll(w3[third, c // 4], nz - (4 * ((c % 4) * nx + x) + 2), 1)
            grads[3 * c, q] = vx[c, q + 2] - vx[c, q]
            grads[3 * c + 1, q] = along_y(V, yr[0, q, c], yr[1, q, c])
            grads[3 * c + 2, q] = along_z(V, T)
        return carry

    lax.fori_loop(0, nx + 2, inside, 0)

    def sides(s, carry):
        sign = jnp.where(s == 0, jnp.float32(1.0), jnp.float32(-1.0))
        E = jnp.where(lane % 2 == 0, ryz[s, 0, 2], ryz[s, 1, 2])
        for c in range(6):
            B = ry[s, 2 * c]
            grads[3 * c, nx + 2 + s] = along_y(B, yr[s, 0, c], yr[s, nx + 1, c])
            grads[3 * c + 1, nx + 2 + s] = sign * (sy[s, 2 * c] - ry[s, 2 * c + 1])
            grads[3 * c + 2, nx + 2 + s] = along_z(B, spin(E, -(2 * c + 1), 1))
        return carry

    lax.fori_loop(0, 2, sides, 0)

    spot = (lane // 4) % nx
    turn = 4 * (nx - 1)
    for h in range(2):
        O, W = sz[0, h], w3[1, h]
        dz = jnp.where(quad == 1, spin(O, -1, 1) - spin(W, 1, 1), spin(W, -1, 1) - spin(O, 1, 1))
        down = jnp.where(spot == 0, spin(w3[0, h], -turn, 1), spin(W, 4, 1))
        up = jnp.where(spot == nx - 1, spin(w3[2, h], turn, 1), spin(W, -4, 1))
        before = jnp.where(is_left, ryz[0, 0, h], ryz[0, 1, h])
        after = jnp.where(is_left, ryz[1, 0, h], ryz[1, 1, h])
        packed = (up - down, along_y(W, before, after), dz)
        for c in range(4 * h, min(4 * h + 4, 6)):
            for j in range(3):
                grads[3 * c + j, nx + 4] = spin(packed[j], -4 * nx * (c % 4), 1)
    phases[nx + 4] = spin(w3[1, 1], -4 * nx * 3, 1)

    def stresses(q, carry):
        g = [[grads[3 * c + j, q] for j in range(3)] for c in range(6)]
        fields = stress_fields(
            twice_rates(g[:3]), twice_rates(g[3:]), phases[q], params, range(6), masks[q]
        )
        for f in range(6):
            for i in range(6):
                stress[6 * f + i, q] = fields[f][i]
        return carry

    lax.fori_loop(0, nx + 5, stresses, 0)
    loads[4].wait()

    def residuals(x, sums):
        sums = list(sums)
        turn = nz - (4 * x + 2)
        T = pltpu.roll(w3[1, 1], nz - (4 * (2 * nx + x) + 2), 1)
        slopes = (
            px[x + 2] - px[x],
            along_y(px[x + 1], yr[0, x + 1, 6], yr[1, x + 1, 6]),
            along_z(px[x + 1], T),
        )
        for i in range(3):
            a, b, c = (FACE_COMPONENTS[j][i] for j in range(3))
            loading = bx[i, x] - 0.5 * slopes[i]
            divided = []
            for f in range(6):
                dx = stress[6 * f + a, x + 2] - stress[6 * f + a, x]
                dy = along_y(
                    stress[6 * f + b, x + 1],
                    stress[6 * f + b, nx + 2, pl.ds(x, 1), :],
                    stress[6 * f + b, nx + 3, pl.ds(x, 1), :],
                )
                dz = along_z(stress[6 * f + c, x + 1], pltpu.roll(stress[6 * f + c, nx + 4], turn, 1))
                divided.append(dx + dy + dz)
            base = divided[0] + loading
            chosen = None
            for k in range(3, -1, -1):
                residual = divided[2 + k] + loading
                linear = base + step_lengths[k] * divided[1]
                sums[k] = sums[k] + residual * residual
                sums[4 + k] = sums[4 + k] + linear * linear
                chosen = residual if chosen is None else jnp.where(accepted == k, residual, chosen)
            cr_ref[i, x] = chosen
        return tuple(sums)

    sums = lax.fori_loop(0, nx, residuals, (blank,) * 8)

    total = blank
    for k in range(8):
        total = jnp.where(sub == k, jnp.sum(sums[k], axis=0, keepdims=True), total)
    total = jnp.sum(total, axis=1, keepdims=True)
    red[rank] = jnp.sum(jnp.where(lane == sub, total, 0.0), axis=0, keepdims=True)

    def share(k, carry):
        pltpu.make_async_remote_copy(
            src_ref=red.at[rank], dst_ref=red.at[rank], send_sem=red_send, recv_sem=red_recv,
            device_id=mate(k), device_id_type=MESH,
        ).start()
        return carry

    lax.fori_loop(1, devices, share, 0)
    others = red.at[pl.ds(0, devices - 1)]
    cr_out.start()
    pltpu.make_async_copy(others, others, red_recv).wait()
    total = jnp.sum(red[...], axis=0)
    cells = 3.0 * nx * ny * nz * devices
    root = jnp.sqrt(total / cells + tiny_mean)
    norms_ref[0:1, :] = root[:, :4]
    norms_ref[1:2, :] = spin(jnp.broadcast_to(root, (ny, nz)), -4, 1)[0:1, :4]

    pltpu.make_async_copy(others, others, red_send).wait()
    cr_out.wait()
    for o in offs:
        @pl.when(exists(o))
        def _():
            for copy in copies_of(o):
                copy.wait_send()


def finish(accepted_ref, n_ref, v_ref, d_ref, r_ref, norms_ref, cv_ref, cr_ref):
    accepted = accepted_ref[0]
    length = jnp.float32(step_lengths[-1])
    for k in range(len(step_lengths) - 2, -1, -1):
        length = jnp.where(accepted == k, jnp.float32(step_lengths[k]), length)
    cv_ref[...] = v_ref[...] + length * d_ref[...]
    cr_ref[...] = r_ref[...]
    norms_ref[...] = n_ref[...]


def body(velocity, direction, pressure, body_force, phase_ids, creep, exponent, yields, accepted):
    sizes = tuple(lax.axis_size(a) for a in AXES)
    nx = velocity.shape[1]
    tile = velocity.shape[2:]
    row = (1, tile[1])
    vmem = pl.BlockSpec(memory_space=pltpu.VMEM)
    smem = pl.BlockSpec(memory_space=pltpu.SMEM)
    hbm = pl.BlockSpec(memory_space=pl.ANY)

    def scratch(*lead, held=jnp.float32, shape=tile):
        return pltpu.VMEM(lead + shape, held)

    norms, residual = pl.pallas_call(
        functools.partial(kernel, sizes),
        out_shape=(
            jax.ShapeDtypeStruct((2, 4), jnp.float32),
            jax.ShapeDtypeStruct(velocity.shape, jnp.float32),
        ),
        in_specs=[smem] * 4 + [hbm] * 5,
        out_specs=(vmem, hbm),
        scratch_shapes=[
            scratch(3, nx),
            scratch(6, nx + 4), scratch(nx + 2), scratch(nx + 2, held=jnp.int32), scratch(3, nx),
            scratch(2, 14), scratch(2, 2, 6, shape=row), scratch(2, 3),
            scratch(2, 14), scratch(2, nx + 2, 7, shape=row), scratch(2, 2),
            scratch(2, 2, 2), scratch(2, 2, 3),
            scratch(3, 2), scratch(18, nx + 5), scratch(36, nx + 5), scratch(nx + 5), scratch(nx + 5),
            scratch(sizes[0] * sizes[1] * sizes[2], shape=row),
            pltpu.SemaphoreType.DMA((5,)), pltpu.SemaphoreType.DMA,
            pltpu.SemaphoreType.DMA((18, 3)), pltpu.SemaphoreType.DMA((18, 3)),
            pltpu.SemaphoreType.DMA, pltpu.SemaphoreType.DMA,
        ],
        compiler_params=pltpu.CompilerParams(collective_id=0, has_side_effects=True),
    )(creep, exponent, yields, accepted, velocity, direction, pressure, body_force, phase_ids)
    return pl.pallas_call(
        finish,
        out_shape=(
            jax.ShapeDtypeStruct((2, 4), jnp.float32),
            jax.ShapeDtypeStruct(velocity.shape, jnp.float32),
            jax.ShapeDtypeStruct(velocity.shape, jnp.float32),
        ),
        in_specs=[smem] + [vmem] * 4,
        out_specs=(vmem, vmem, vmem),
    )(accepted, norms, velocity, direction, residual)


def solution(mesh):
    placed = (
        P(None, "gx", "gy", "gz"),
        P(None, "gx", "gy", "gz"),
        P("gx", "gy", "gz"),
        P(None, "gx", "gy", "gz"),
        P("gx", "gy", "gz"),
        P(),
        P(),
        P(),
        P(),
    )
    return jax.shard_map(
        body,
        mesh=mesh,
        in_specs=placed,
        out_specs=(P(), P(None, "gx", "gy", "gz"), P(None, "gx", "gy", "gz")),
        check_vma=False,
    )
```
